128 devices in a mesh: data: 1, hid: 16 (over z, y), vocab: 8 (over x, core).
Axes of the slice: x: 4, y: 4, z: 4, core: 2. Of those that a mesh axis runs over, the one named last changes fastest.
Arguments:
- h_states: bfloat16 [1024, 4096], P('data', 'hid')
- w_head: bfloat16 [4096, 32768], P('hid', 'vocab')
- inv_temp: float32 [1024], P('data')
- tgt_ids: int32 [1024], P('data')
Outputs:
- output 1: float32 [1024, 32768], P('data', ('vocab', 'hid'))
- output 2: float32 [1024], P('data')
All inputs are finite; a program needn't handle non-finite values.
Results may differ from the reference program's by a relative error of at most 0.001.
Values are sent between devices in bfloat16 or wider.
A program may use at most 1 GiB of HBM per device.

```python
import jax
import jax.numpy as jnp
from jax import lax
import math

B = 1024
D = 4096
V = 32768


def setup_inputs(seed: int = 0, part: int = 0) -> dict:
    part_keys = jax.random.split(jax.random.fold_in(jax.random.key(seed), part), 5)
    shared_keys = jax.random.split(jax.random.key(seed + 1), 2)
    common_dir = jax.random.normal(shared_keys[0], (D,), jnp.float32)
    col_level = 140.0 - 2.5 * jnp.arange(V, dtype=jnp.float32) / V
    row_keys = jax.random.split(shared_keys[1], D // 128)
    dir_blocks = common_dir.reshape(D // 128, 128)

    def weight_block(block_args):
        blk_key, dir_part = block_args
        noise_blk = jax.random.normal(blk_key, (128, V), jnp.float32)
        w_part = noise_blk * (0.6 / math.sqrt(D)) + dir_part[:, None] * (col_level[None, :] / D)
        return w_part.astype(jnp.bfloat16)

    w_head = lax.map(weight_block, (row_keys, dir_blocks)).reshape(D, V)
    row_noise = jax.random.normal(part_keys[0], (B, D), jnp.float32)
    row_shift = jax.random.uniform(part_keys[1], (B,), jnp.float32, 1.0, 2.0)
    h_states = (row_noise + row_shift[:, None] * common_dir[None, :]).astype(jnp.bfloat16)
    inv_temp = jax.random.uniform(part_keys[2], (B,), jnp.float32, 0.7, 1.3)
    first_pick = jax.random.randint(part_keys[3], (B,), 0, V)
    second_pick = jax.random.randint(part_keys[4], (B,), 0, V)
    tgt_ids = jnp.maximum(first_pick, second_pick).at[0].set(0).at[1].set(V - 1)
    return {"h_states": h_states, "w_head": w_head, "inv_temp": inv_temp, "tgt_ids": tgt_ids}


def reference(h_states, w_head, inv_temp, tgt_ids):
    logits = jnp.dot(h_states, w_head, preferred_element_type=jnp.float32) * inv_temp[:, None]
    row_max = jnp.max(logits, axis=1, keepdims=True)
    exp_vals = jnp.exp(logits - row_max)
    row_sum = jnp.sum(exp_vals, axis=1, keepdims=True)
    prob_rows = exp_vals / row_sum
    cdf_table = jnp.cumsum(prob_rows, axis=1)
    cdf_at_tgt = jnp.take_along_axis(cdf_table, tgt_ids[:, None], axis=1)[:, 0]
    return (cdf_table, cdf_at_tgt)
```

```python
import functools

import jax
import jax.numpy as jnp
from jax import lax
from jax.experimental import pallas as pl
from jax.experimental.pallas import tpu as pltpu
from jax.sharding import PartitionSpec as P

MESH = pl.DeviceIdType.MESH
BF = jnp.bfloat16
F32 = jnp.float32

B = 1024
KB = 256
TB = 256
PC = 64


def _mod4(a):
    return lax.rem(a, 4)


def _kernel(h_ref, w_ref, temp_ref, tgt_ref, cum_ref, so_ref, at_ref,
            H, Wsrc, Wv, cum, tcol, gcol, St, G1, S2, G2,
            loc, r1, r2, r3, rx, rxr, rd, rw, rs1, rs2, ss):
    hid = lax.axis_index("hid")
    voc = lax.axis_index("vocab")
    z, y, x, c = hid // 4, _mod4(hid), voc // 2, lax.rem(voc, 2)

    def dev(dz=0, dy=0, dx=0, dc=0):
        return {"hid": _mod4(z + dz) * 4 + _mod4(y + dy),
                "vocab": _mod4(x + dx) * 2 + lax.rem(c + dc, 2)}

    plane = [(a, b) for a in range(4) for b in range(4) if a or b]
    column = [(a, b) for a in range(4) for b in range(2) if a or b]

    barrier = pltpu.get_barrier_semaphore()
    for a, b in plane:
        pl.semaphore_signal(barrier, inc=1, device_id=dev(a, b), device_id_type=MESH)
    for a, b in column:
        pl.semaphore_signal(barrier, inc=1, device_id=dev(0, 0, a, b), device_id_type=MESH)

    own_h = pltpu.make_async_copy(h_ref, H.at[z, y], loc.at[0])
    own_h.start()
    all_w = pltpu.make_async_copy(w_ref, Wsrc, loc.at[1])
    all_w.start()
    own_w = pltpu.make_async_copy(
        w_ref.at[:, pl.ds(pl.multiple_of(hid * TB, TB), TB)],
        Wv.at[pl.ds(pl.multiple_of(hid * KB, KB), KB)], loc.at[2])
    own_w.start()

    for g in range(8):
        tcol[pl.ds(g * 128, 128), :] = jnp.broadcast_to(temp_ref[g:g + 1, :], (128, 128)).T
        gcol[pl.ds(g * 128, 128), :] = jnp.broadcast_to(tgt_ref[g:g + 1, :].astype(F32), (128, 128)).T

    pl.semaphore_wait(barrier, len(plane) + len(column))
    own_h.wait()

    def rows(p, dx=0, dc=0):
        return pl.ds(pl.multiple_of(_mod4(x + dx) * 256 + lax.rem(c + dc, 2) * 128 + p * PC, PC), PC)

    def single(p, f, s, dx=0, dc=0):
        dz, dy = (s, f) if p == 0 else (f, s)
        return H.at[_mod4(z + dz), _mod4(y + dy), rows(p, dx, dc), :]

    def group(p, s, dx=0, dc=0):
        if p == 0:
            return H.at[_mod4(z + s), :, rows(p, dx, dc), :]
        return H.at[:, _mod4(y + s), rows(p, dx, dc), :]

    def send(ref, to, recv_sem, cat):
        pltpu.make_async_remote_copy(src_ref=ref, dst_ref=ref, send_sem=ss.at[cat], recv_sem=recv_sem,
                                     device_id=to, device_id_type=MESH).start()

    def got(ref, sem):
        pltpu.make_async_copy(ref, ref, sem).wait()

    def first_dev(p, d):
        return dev(0, d) if p == 0 else dev(d, 0)

    def second_dev(p, d):
        return dev(d, 0) if p == 0 else dev(0, d)

    def send_w(a, b):
        peer = _mod4(z + a) * 4 + _mod4(y + b)
        pltpu.make_async_remote_copy(
            src_ref=Wsrc.at[:, pl.ds(pl.multiple_of(peer * TB, TB), TB)],
            dst_ref=Wv.at[pl.ds(pl.multiple_of(hid * KB, KB), KB)],
            send_sem=ss.at[3], recv_sem=rw.at[a * 4 + b], device_id=dev(a, b), device_id_type=MESH).start()

    def part(p, g, dx=0, dc=0):
        if g < 3:
            return single(p, (1, 3, 2)[g], 0, dx, dc)
        return group(p, (1, 3, 2)[g - 3], dx, dc)

    def to_partner(p, g, src):
        ref = part(p, g, src, 0)
        send(ref, dev(0, 0, 0, 1), rd.at[p, src, g], 2)

    def spread(p, g):
        ref = part(p, g)
        send(ref, dev(0, 0, 1), rx.at[p, 0, g], 1)
        send(ref, dev(0, 0, 3), rx.at[p, 1, g], 1)
        to_partner(p, g, 0)

    for p in range(2):
        me = single(p, 0, 0)
        for d in (1, 3, 2):
            send(me, first_dev(p, d), r1.at[p, d - 1], 0)
    for p in range(2):
        me = single(p, 0, 0)
        send(me, second_dev(p, 1), r2.at[p, 0, 0], 0)
        send(me, second_dev(p, 3), r2.at[p, 1, 0], 0)
    all_w.wait()
    order = [(0, 1), (0, 3), (1, 0), (3, 0), (1, 1), (3, 3), (1, 3), (3, 1),
             (0, 2), (2, 0), (1, 2), (2, 1), (3, 2), (2, 3), (2, 2)]
    for a, b in order[:4]:
        send_w(a, b)
    for i, d in enumerate((1, 3, 2)):
        for p in range(2):
            ref = single(p, d, 0)
            got(ref, r1.at[p, (4 - d) - 1])
            send(ref, second_dev(p, 1), r2.at[p, 0, d], 0)
            send(ref, second_dev(p, 3), r2.at[p, 1, d], 0)
            spread(p, i)
    for a, b in order[4:6]:
        send_w(a, b)
    for j in range(4):
        for p in range(2):
            for way, s in ((0, 3), (1, 1)):
                ref = single(p, j, s)
                got(ref, r2.at[p, way, j])
                if j % 2 == way:
                    send(ref, second_dev(p, 1 if way == 0 else 3), r3.at[p, j], 0)
    for p in range(2):
        spread(p, 3)
        spread(p, 4)
    for a, b in order[6:]:
        send_w(a, b)
    for p in range(2):
        for j in range(4):
            got(single(p, j, 2), r3.at[p, j])
        spread(p, 5)

    def from_x(g):
        for p in range(2):
            for way, dx in ((0, 3), (1, 1)):
                ref = part(p, g, dx)
                got(ref, rx.at[p, way, g])
                if p == way:
                    send(ref, dev(0, 0, 1 if way == 0 else 3), rxr.at[p, g], 1)
                to_partner(p, g, dx)

    def from_far(g):
        for p in range(2):
            got(part(p, g, 2), rxr.at[p, g])
            to_partner(p, g, 2)

    base = ((voc * 16 + hid) * TB).astype(F32)
    lane = lax.broadcasted_iota(jnp.int32, (128, 128), 1)
    col = lax.broadcasted_iota(jnp.int32, (256, TB), 1).astype(F32)
    tri = (lax.broadcasted_iota(jnp.int32, (TB, TB), 0) <= lax.broadcasted_iota(jnp.int32, (TB, TB), 1)).astype(F32).astype(BF)
    tri3 = jnp.concatenate([tri, tri, tri], axis=0)

    def compute(dx):
        for p in range(2):
            for g in range(6):
                got(part(p, g, dx, 1), rd.at[p, dx, g])
        q = _mod4(x + dx)
        rr = pl.ds(pl.multiple_of(q * 256, 256), 256)
        lhs = jnp.concatenate([H[k // 4, k % 4, rr, :] for k in range(16)], axis=1)
        zz = jnp.dot(lhs, Wv[...], preferred_element_type=F32)
        tc = tcol[rr, :]
        zz = zz * jnp.concatenate([tc, tc], axis=1)
        m = jnp.max(zz, axis=1, keepdims=True)
        e = jnp.exp(zz - m)
        e1 = e.astype(BF)
        f1 = e - e1.astype(F32)
        e2 = f1.astype(BF)
        e3 = (f1 - e2.astype(F32)).astype(BF)
        cs = jnp.dot(jnp.concatenate([e1, e2, e3], axis=1), tri3, preferred_element_type=F32)
        cum[rr, :] = cs
        gc = gcol[rr, :] - base
        t = jnp.sum(jnp.where(col <= jnp.concatenate([gc, gc], axis=1), e, 0.0), axis=1, keepdims=True)
        s = cs[:, TB - 1:TB]
        for i in range(2):
            a = slice(i * 128, (i + 1) * 128)
            pk = jnp.where(lane == 0, m[a], jnp.where(lane == 1, s[a], t[a])).T
            for k in range(3):
                St[k, pl.ds(q * 2 + i, 1), :] = pk[k:k + 1, :]
        pltpu.make_async_copy(cum.at[rr], cum_ref.at[rr], loc.at[3]).start()

    for g in range(6):
        from_x(g)
    own_w.wait()
    for a, b in plane:
        sender = _mod4(z + 4 - a) * 4 + _mod4(y + 4 - b)
        got(Wv.at[pl.ds(pl.multiple_of(sender * KB, KB), KB)], rw.at[a * 4 + b])
    compute(0)
    for g in range(3):
        from_far(g)
    compute(3)
    for g in range(3, 5):
        from_far(g)
    compute(1)
    from_far(5)
    compute(2)

    G1[hid] = St[...]
    for a, b in plane:
        pltpu.make_async_remote_copy(src_ref=St, dst_ref=G1.at[hid], send_sem=ss.at[4], recv_sem=rs1.at[a * 4 + b],
                                     device_id=dev(a, b), device_id_type=MESH).start()
    for a, b in plane:
        got(G1.at[_mod4(z + 4 - a) * 4 + _mod4(y + 4 - b)], rs1.at[a * 4 + b])
    mv = G1[0, 0]
    for k in range(1, 16):
        mv = jnp.maximum(mv, G1[k, 0])
    sv = jnp.zeros((8, 128), F32)
    pre = jnp.zeros((8, 128), F32)
    tv = jnp.zeros((8, 128), F32)
    for k in range(16):
        f = jnp.exp(G1[k, 0] - mv)
        sk = G1[k, 1] * f
        sv += sk
        tv += G1[k, 2] * f
        pre += jnp.where(k < hid, sk, 0.0)
    S2[0] = mv
    S2[1] = sv
    S2[2] = tv
    G2[voc] = S2[...]
    for a, b in column:
        pltpu.make_async_remote_copy(src_ref=S2, dst_ref=G2.at[voc], send_sem=ss.at[5], recv_sem=rs2.at[a * 2 + b],
                                     device_id=dev(0, 0, a, b), device_id_type=MESH).start()
    for a, b in column:
        got(G2.at[_mod4(x + 4 - a) * 2 + lax.rem(c + b, 2)], rs2.at[a * 2 + b])
    mx = G2[0, 0]
    for k in range(1, 8):
        mx = jnp.maximum(mx, G2[k, 0])
    tot = jnp.zeros((8, 128), F32)
    below = jnp.zeros((8, 128), F32)
    at = jnp.zeros((8, 128), F32)
    for k in range(8):
        f = jnp.exp(G2[k, 0] - mx)
        sk = G2[k, 1] * f
        tot += sk
        at += G2[k, 2] * f
        below += jnp.where(k < voc, sk, 0.0)
    so_ref[0] = jnp.exp(St[0] - mx) / tot
    so_ref[1] = (pre * jnp.exp(mv - mx) + below) / tot
    at_ref[...] = at / tot

    pltpu.make_async_copy(cum, cum_ref, loc.at[3]).wait()
    got(H.at[0:3, 0:4, 0:160, :], ss.at[0])
    got(H.at[0:3, 0:4, 0:480, :], ss.at[1])
    got(H.at[0:3, 0:4, 0:640, :], ss.at[2])
    got(Wv.at[0:15 * KB], ss.at[3])
    got(G1.at[0:15], ss.at[4])
    got(G2.at[0:7], ss.at[5])


def solution(mesh):
    dma = pltpu.SemaphoreType.DMA
    call = pl.pallas_call(
        _kernel,
        name="head_cdf",
        out_shape=(jax.ShapeDtypeStruct((B, TB), F32),
                   jax.ShapeDtypeStruct((2, 8, 128), F32),
                   jax.ShapeDtypeStruct((8, 128), F32)),
        in_specs=[pl.BlockSpec(memory_space=pl.ANY), pl.BlockSpec(memory_space=pl.ANY),
                  pl.BlockSpec(memory_space=pltpu.VMEM), pl.BlockSpec(memory_space=pltpu.VMEM)],
        out_specs=(pl.BlockSpec(memory_space=pl.ANY), pl.BlockSpec(memory_space=pltpu.VMEM),
                   pl.BlockSpec(memory_space=pltpu.VMEM)),
        scratch_shapes=[
            pltpu.VMEM((4, 4, B, KB), BF),
            pltpu.VMEM((KB, 4096), BF),
            pltpu.VMEM((4096, TB), BF),
            pltpu.VMEM((B, TB), F32),
            pltpu.VMEM((B, 128), F32),
            pltpu.VMEM((B, 128), F32),
            pltpu.VMEM((3, 8, 128), F32),
            pltpu.VMEM((16, 3, 8, 128), F32),
            pltpu.VMEM((3, 8, 128), F32),
            pltpu.VMEM((8, 3, 8, 128), F32),
            dma((5,)), dma((2, 3)), dma((2, 2, 4)), dma((2, 4)), dma((2, 2, 6)), dma((2, 6)), dma((2, 4, 6)),
            dma((16,)), dma((16,)), dma((8,)), dma((6,)),
        ],
        compiler_params=pltpu.CompilerParams(collective_id=0, has_side_effects=True, vmem_limit_bytes=48 * 2**20),
    )

    def local(h_blk, w_blk, temp, tgt):
        cum, so, at = call(h_blk, w_blk, temp.reshape(8, 128), tgt.reshape(8, 128))
        so = so.reshape(2, B)
        return cum * so[0][:, None] + so[1][:, None], at.reshape(B)

    return jax.shard_map(local, mesh=mesh,
                         in_specs=(P("data", "hid"), P("hid", "vocab"), P("data"), P("data")),
                         out_specs=(P("data", ("vocab", "hid")), P("data")), check_vma=False)
```
